256 devices in a mesh: freq: 8 (over z), tile: 32 (over x, y, core).
Axes of the slice: x: 4, y: 4, z: 8, core: 2. Of those that a mesh axis runs over, the one named last changes fastest.
Arguments:
- signal: bfloat16 [8, 2, 128, 16384], P('freq', None, None, 'tile'), may hold values from -6 to 6
- v_factors: bfloat16 [8, 64, 2, 48, 16384], P('freq', None, None, None, 'tile'), may hold values from -0.375 to 0.375
- u_factors: bfloat16 [8, 64, 2, 48, 16384], P('freq', None, None, None, 'tile'), may hold values from -0.0546875 to 0.0546875
- tile_ranks: int32 [8, 64, 64], P('freq'), may hold values from 16 to 48
- row_order: int32 [64], replicated, may hold values from 0 to 63, each once
- col_order: int32 [64], replicated, may hold values from 0 to 63, each once
- time_gate: float32 [2, 8, 8], replicated, may hold values from -1.5 to 1.5
Outputs:
- forward_data: bfloat16 [8, 2, 128, 16384], P('freq', None, None, 'tile')
- adjoint_data: bfloat16 [8, 2, 128, 16384], P('freq', None, None, 'tile')
The draws below stay inside these ranges and needn't reach their ends.
Inputs may be any that keep to these rules, and one draw needn't show every extreme that they name: tile_ranks[f, i, j] is the rank of kernel tile (i, j) at frequency f. `row_order`: a permutation of the 64 kernel tile rows. `col_order`: a permutation of the 64 kernel tile columns.
All inputs are finite; a program needn't handle non-finite values.
Results may differ from the reference program's by a relative error of at most 0.0075.
Values may be sent and summed in bfloat16 or wider, within the bound.
A program may use at most 128 MiB of HBM per device.

```python
import jax
import jax.numpy as jnp
from jax import lax

TILE = 256
RMAX = 48
RMIN = 16
SRC = 128
TR = 64
TC = 64
M = 16384
N = 16384
FREQS = 8


def with_ends(array, key, least, top_value):
    place = [jax.random.randint(jax.random.fold_in(key, axis), (), 0, length) for axis, length in enumerate(array.shape)]
    longest = array.shape.index(max(array.shape))
    neighbour = place[:longest] + [(place[longest] + 1) % array.shape[longest]] + place[longest + 1:]
    return array.at[tuple(place)].set(least).at[tuple(neighbour)].set(top_value)


def level_of(stream_key, extent, pieces, low, high):
    def one(dim, shards_of):
        steps = jax.random.uniform(jax.random.fold_in(jax.random.fold_in(stream_key, 6), dim), (shards_of,), jnp.float32, low / len(pieces), high / len(pieces))
        return jnp.repeat(jnp.exp(steps), extent[dim] // shards_of).reshape((-1,) + (1,) * (len(extent) - dim - 1))

    gain = one(*pieces[0])
    for cut in pieces[1:]:
        gain = gain * one(*cut)
    return gain


def gaussian(own_key, dims, width, most, split=(), held_as=jnp.bfloat16):
    values = jax.random.normal(own_key, dims, jnp.float32) * width
    if len(split) > 0:
        values = level_of(own_key, dims, split, -0.22, 0.18) * values
    return jnp.clip(values, min=-most, max=most).astype(held_as)


def setup_inputs(seed: int = 0) -> dict:
    key_list = jax.random.split(jax.random.key(seed), 8)
    return {
        "signal": gaussian(key_list[0], (FREQS, 2, SRC, N), 1.0, 6.0, ((0, 8), (3, 32))),
        "v_factors": gaussian(key_list[1], (FREQS, TR, 2, RMAX, N), TILE ** -0.5, 0.375, ((0, 8), (4, 32))),
        "u_factors": gaussian(key_list[2], (FREQS, TC, 2, RMAX, M), (4 * TC * RMAX) ** -0.5, 0.0546875, ((0, 8), (4, 32))),
        "tile_ranks": with_ends(jax.random.randint(key_list[3], (FREQS, TR, TC), RMIN, RMAX + 1), jax.random.fold_in(key_list[3], 1), RMIN, RMAX).astype(jnp.int32),
        "row_order": jax.random.permutation(key_list[4], TR).astype(jnp.int32),
        "col_order": jax.random.permutation(key_list[5], TC).astype(jnp.int32),
        "time_gate": gaussian(key_list[6], (2, FREQS, FREQS), (2 * FREQS) ** -0.5, 1.5, (), jnp.float32),
    }


def combine(product, conjugate, stack_axis):
    if conjugate:
        real_part = product[0, 0] + product[1, 1]
        imag_part = product[0, 1] - product[1, 0]
    else:
        real_part = product[0, 0] - product[1, 1]
        imag_part = product[0, 1] + product[1, 0]
    return jnp.stack([real_part, imag_part], axis=stack_axis)


def reference(signal, v_factors, u_factors, tile_ranks, row_order, col_order, time_gate):
    stored = tile_ranks[:, row_order][:, :, col_order]
    rank_slots = jnp.arange(RMAX, dtype=jnp.int32)

    def forward_one(inputs):
        sig, right, left, ranks_here = inputs
        live_mask = (rank_slots[None, None, :] < ranks_here[:, :, None]).astype(jnp.float32)
        right_full = right.astype(jnp.float32).reshape(TR, 2, RMAX, TC, TILE)
        sources = sig.astype(jnp.float32).reshape(2, SRC, TC, TILE)
        product = jnp.einsum('kprlt,qslt->pqklrs', right_full, sources)
        coefficients = (combine(product, False, 0) * live_mask[None, :, :, :, None]).astype(jnp.bfloat16)
        left_full = left.astype(jnp.float32).reshape(TC, 2, RMAX, TR, TILE)
        product = jnp.einsum('lqrkt,pklrs->qpskt', left_full, coefficients.astype(jnp.float32))
        return combine(product, False, 0).reshape(2, SRC, M).astype(jnp.bfloat16)

    forward_all = lax.map(forward_one, (signal, v_factors, u_factors, stored))
    product = jnp.einsum('pfe,eqsm->pqfsm', time_gate, forward_all.astype(jnp.float32),
                         precision=lax.Precision.HIGHEST)
    gated_all = combine(product, False, 1).astype(jnp.bfloat16)

    def adjoint_one(inputs):
        gated_rows, right, left, ranks_here = inputs
        live_mask = (rank_slots[None, None, :] < ranks_here[:, :, None]).astype(jnp.float32)
        left_full = left.astype(jnp.float32).reshape(TC, 2, RMAX, TR, TILE)
        rows_here = gated_rows.astype(jnp.float32).reshape(2, SRC, TR, TILE)
        product = jnp.einsum('lqrkt,pskt->qpklrs', left_full, rows_here)
        adjoint_coef = (combine(product, True, 0) * live_mask[None, :, :, :, None]).astype(jnp.bfloat16)
        right_full = right.astype(jnp.float32).reshape(TR, 2, RMAX, TC, TILE)
        product = jnp.einsum('kqrlt,pklrs->qpslt', right_full, adjoint_coef.astype(jnp.float32))
        return combine(product, True, 0).reshape(2, SRC, N).astype(jnp.bfloat16)

    adjoint_all = lax.map(adjoint_one, (gated_all, v_factors, u_factors, stored))
    return forward_all, adjoint_all
```

```python
import functools

import jax
import jax.numpy as jnp
from jax import lax
from jax.experimental import pallas as pl
from jax.experimental.pallas import tpu as pltpu
from jax.sharding import PartitionSpec as P

MESH = pl.DeviceIdType.MESH
NX, NY, NC = 4, 4, 2
NT = NX * NY * NC
NF = 8
TILE = 256
RMAX = 48
SRC = 128
HS = SRC // 2
HL = 2 * HS
GD = NT // NX
GROWS = GD * 2 * RMAX


def kernel(
    sig_hbm, v_hbm, u_hbm, ranks, row_order, col_order, gate,
    fwd_hbm, adj_hbm,
    sig, v, u, w, b, send1, recv1, send2, recv2, acc, zs, zr, gs, gr, fo, ao,
    sem_sig, sem_v, sem_u, sem_out,
    s1_send, s1_recv, s2_send, s2_recv, z1_send, z1_recv, z2_send, z2_recv,
):
    fr = lax.axis_index("freq")
    me = lax.axis_index("tile")
    core = lax.rem(me, NC)
    y = lax.rem(me // NC, NY)
    x = me // (NC * NY)

    sig_copy = pltpu.make_async_copy(sig_hbm.at[0], sig, sem_sig)
    sig_copy.start()

    def v_copy(g):
        rows = pl.ds(g * 16, 16)
        return pltpu.make_async_copy(v_hbm.at[0, rows], v.at[rows], sem_v.at[g])

    for i in range(NX):
        v_copy(lax.rem(x + 1 + i, NX)).start()
    u_copy = pltpu.make_async_copy(u_hbm.at[0], u, sem_u)
    u_copy.start()

    barrier = pltpu.get_barrier_semaphore()

    def greet_tile(d, carry):
        pl.semaphore_signal(
            barrier, inc=1, device_id=(fr, lax.rem(me + d, NT)), device_id_type=MESH
        )
        return carry

    def greet_freq(d, carry):
        pl.semaphore_signal(
            barrier, inc=1, device_id=(lax.rem(fr + d, NF), me), device_id_type=MESH
        )
        return carry

    lax.fori_loop(1, NT, greet_tile, 0)
    lax.fori_loop(1, NF, greet_freq, 0)

    sig_copy.wait()
    for l in range(2):
        cols = pl.ds(l * TILE, TILE)
        for h in range(2):
            src = pl.ds(h * HS, HS)
            re = sig[0, src, cols]
            im = sig[1, src, cols]
            w[l, pl.ds(h * HL, HS), pl.ds(0, TILE)] = re
            w[l, pl.ds(h * HL + HS, HS), pl.ds(0, TILE)] = im
            w[l, pl.ds(h * HL, HS), pl.ds(TILE, TILE)] = -im
            w[l, pl.ds(h * HL + HS, HS), pl.ds(TILE, TILE)] = re

    slots = lax.broadcasted_iota(jnp.int32, (RMAX, 1), 0)

    def stage1(g):
        for l in range(2):
            col = col_order[me * 2 + l]
            cols = pl.ds(l * TILE, TILE)
            lhs = jnp.concatenate(
                [v[pl.ds(g * 16, 16), p, :, cols].reshape(GROWS, TILE) for p in range(2)], axis=1
            )
            out = lax.dot_general(
                lhs, w[l], (((1,), (1,)), ((), ())), preferred_element_type=jnp.float32
            )
            for k in range(16):
                rank = ranks[0, row_order[g * 16 + k], col]
                part = out[k * RMAX : (k + 1) * RMAX]
                part = jnp.where(slots < rank, part, 0.0).astype(jnp.bfloat16)
                for h in range(2):
                    send1[h, g * GD + k // 2, k % 2, l] = part[:, h * HL : (h + 1) * HL]

    def peer(dx, t, dc):
        px = lax.rem(x + dx, NX)
        py = lax.rem(y + dx + t, NY)
        return (px * NY + py) * NC + lax.rem(core + dc, NC)

    def tile_copy(send, recv, sems, rsems, h, other):
        return pltpu.make_async_remote_copy(
            src_ref=send.at[h, other],
            dst_ref=recv.at[h, me],
            send_sem=sems.at[h, other],
            recv_sem=rsems.at[h, me],
            device_id=(fr, other),
            device_id_type=MESH,
        )

    def arrival(send, recv, sems, rsems, h, other):
        return pltpu.make_async_remote_copy(
            src_ref=send.at[h, other],
            dst_ref=recv.at[h, other],
            send_sem=sems.at[h, other],
            recv_sem=rsems.at[h, other],
            device_id=(fr, other),
            device_id_type=MESH,
        )

    ex1 = (send1, recv1, s1_send, s1_recv)
    ex2 = (send2, recv2, s2_send, s2_recv)

    def send_all(ex, h):
        def body(i, carry):
            tile_copy(*ex, h, peer(lax.rem(i, 4), lax.rem(i // 4, 4), i // 16)).start()
            return carry

        lax.fori_loop(1, NT, body, 0)

    def wait_sends(ex, h):
        def body(d, carry):
            arrival(*ex, h, lax.rem(me + d, NT)).wait_send()
            return carry

        lax.fori_loop(1, NT, body, 0)

    def wait_group(ex, h, g):
        def body(i, carry):
            other = g * GD + i

            @pl.when(other != me)
            def _():
                arrival(*ex, h, other).wait_recv()

            return carry

        lax.fori_loop(0, GD, body, 0)

    def first_group(i, carry):
        g = lax.rem(x + 1 + i, NX)
        v_copy(g).wait()
        stage1(g)
        return carry

    lax.fori_loop(0, NX, first_group, 0)
    pl.semaphore_wait(barrier, NT - 1 + NF - 1)
    send_all(ex1, 0)
    send_all(ex1, 1)
    for h in range(2):
        recv1[h, me] = send1[h, me]

    def expand(ex, factor, h):
        recv = ex[1]

        def body(i, carry):
            g = lax.rem(x + i, NX)
            wait_group(ex, h, g)
            for j in range(2):
                cols = pl.ds(j * TILE, TILE)
                c = recv[h, pl.ds(g * GD, GD), j].reshape(GROWS, HL)
                rhs = jnp.concatenate(
                    [factor[pl.ds(g * 16, 16), p, :, cols].reshape(GROWS, TILE) for p in range(2)],
                    axis=1,
                )
                term = lax.dot_general(
                    c, rhs, (((0,), (0,)), ((), ())), preferred_element_type=jnp.float32
                )

                @pl.when(i == 0)
                def _():
                    acc[j] = term

                @pl.when(i > 0)
                def _():
                    acc[j] += term

            return carry

        lax.fori_loop(0, NX, body, 0)

    def z_copy(src, dst, sems, rsems, h, other, slot):
        return pltpu.make_async_remote_copy(
            src_ref=src.at[h, other],
            dst_ref=dst.at[h, slot],
            send_sem=sems.at[h, other],
            recv_sem=rsems.at[h, slot],
            device_id=(other, me),
            device_id_type=MESH,
        )

    def z_exchange(src, dst, sems, rsems, h):
        def start(d, carry):
            z_copy(src, dst, sems, rsems, h, lax.rem(fr + d, NF), fr).start()
            return carry

        def finish(d, carry):
            other = lax.rem(fr + d, NF)
            z_copy(src, dst, sems, rsems, h, other, other).wait()
            return carry

        lax.fori_loop(1, NF, start, 0)
        dst[h, fr] = src[h, fr]
        lax.fori_loop(1, NF, finish, 0)

    u_copy.wait()
    fwd_copies = []
    for h in range(2):
        expand(ex1, u, h)
        rows = pl.ds(h * HS, HS)
        for j in range(2):
            cols = pl.ds(j * TILE, TILE)
            re = (acc[j, 0:HS, 0:TILE] - acc[j, HS:HL, TILE:]).astype(jnp.bfloat16)
            im = (acc[j, HS:HL, 0:TILE] + acc[j, 0:HS, TILE:]).astype(jnp.bfloat16)
            fo[0, rows, cols] = re
            fo[1, rows, cols] = im
            for n in range(2):
                for m in range(2):
                    f = m * 4 + j * 2 + n
                    zs[h, f, 0] = re[m * 32 : m * 32 + 32, n * 128 : n * 128 + 128]
                    zs[h, f, 1] = im[m * 32 : m * 32 + 32, n * 128 : n * 128 + 128]
        z_exchange(zs, zr, z1_send, z1_recv, h)

        def gate_rows(i, carry):
            rs = pl.ds(pl.multiple_of(i * 16, 16), 16)
            parts = [
                [zr[h, e, q, rs, :].astype(jnp.float32) for q in range(2)] for e in range(NF)
            ]
            for f in range(NF):
                re = jnp.zeros((16, 128), jnp.float32)
                im = jnp.zeros((16, 128), jnp.float32)
                for e in range(NF):
                    a, c = gate[0, f, e], gate[1, f, e]
                    re += a * parts[e][0] - c * parts[e][1]
                    im += a * parts[e][1] + c * parts[e][0]
                gs[h, f, 0, rs, :] = re.astype(jnp.bfloat16)
                gs[h, f, 1, rs, :] = im.astype(jnp.bfloat16)
            return carry

        lax.fori_loop(0, 2, gate_rows, 0)
        z_exchange(gs, gr, z2_send, z2_recv, h)

        for e in range(NF):
            m, j, n = e // 4, (e % 4) // 2, e % 2
            re = gr[h, e, 0]
            im = gr[h, e, 1]
            low = pl.ds(m * 32, 32)
            high = pl.ds(HS + m * 32, 32)
            b[j, low, pl.ds(n * 128, 128)] = re
            b[j, high, pl.ds(n * 128, 128)] = im
            b[j, low, pl.ds(TILE + n * 128, 128)] = im
            b[j, high, pl.ds(TILE + n * 128, 128)] = -re

        def stage3(g, carry):
            for j in range(2):
                row = row_order[me * 2 + j]
                cols = pl.ds(j * TILE, TILE)
                lhs = jnp.concatenate(
                    [u[pl.ds(g * 16, 16), p, :, cols].reshape(GROWS, TILE) for p in range(2)],
                    axis=1,
                )
                out = lax.dot_general(
                    lhs, b[j], (((1,), (1,)), ((), ())), preferred_element_type=jnp.float32
                )
                for k in range(16):
                    rank = ranks[0, row, col_order[g * 16 + k]]
                    part = out[k * RMAX : (k + 1) * RMAX]
                    part = jnp.where(slots < rank, part, 0.0).astype(jnp.bfloat16)
                    send2[h, g * GD + k // 2, k % 2, j] = part
            return carry

        lax.fori_loop(0, NX, stage3, 0)
        send_all(ex2, h)
        recv2[h, me] = send2[h, me]

    fwd_copy = pltpu.make_async_copy(fo, fwd_hbm.at[0], sem_out.at[0])
    fwd_copy.start()
    for h in range(2):
        expand(ex2, v, h)
        rows = pl.ds(h * HS, HS)
        for j in range(2):
            cols = pl.ds(j * TILE, TILE)
            ao[0, rows, cols] = (acc[j, 0:HS, 0:TILE] + acc[j, HS:HL, TILE:]).astype(jnp.bfloat16)
            ao[1, rows, cols] = (acc[j, HS:HL, 0:TILE] - acc[j, 0:HS, TILE:]).astype(jnp.bfloat16)
    adj_copy = pltpu.make_async_copy(ao, adj_hbm.at[0], sem_out.at[1])
    adj_copy.start()
    for h in range(2):
        wait_sends(ex1, h)
        wait_sends(ex2, h)
    fwd_copy.wait()
    adj_copy.wait()


def shards(signal, v_factors, u_factors, tile_ranks, row_order, col_order, time_gate):
    bf16, f32 = jnp.bfloat16, jnp.float32
    block = (2, NT, 2, 2, RMAX, HL)
    hbm = pl.BlockSpec(memory_space=pl.ANY)
    smem = pl.BlockSpec(memory_space=pltpu.SMEM)
    dma = pltpu.SemaphoreType.DMA
    out = jax.ShapeDtypeStruct((1, 2, SRC, 2 * TILE), bf16)
    return pl.pallas_call(
        kernel,
        out_shape=(out, out),
        in_specs=[hbm, hbm, hbm, smem, smem, smem, smem],
        out_specs=(hbm, hbm),
        scratch_shapes=[
            pltpu.VMEM((2, SRC, 2 * TILE), bf16),
            pltpu.VMEM(v_factors.shape[1:], bf16),
            pltpu.VMEM(u_factors.shape[1:], bf16),
            pltpu.VMEM((2, 2 * SRC, 2 * TILE), bf16),
            pltpu.VMEM((2, HL, 2 * TILE), bf16),
            pltpu.VMEM(block, bf16),
            pltpu.VMEM(block, bf16),
            pltpu.VMEM(block, bf16),
            pltpu.VMEM(block, bf16),
            pltpu.VMEM((2, HL, 2 * TILE), f32),
            pltpu.VMEM((2, NF, 2, 32, 128), bf16),
            pltpu.VMEM((2, NF, 2, 32, 128), bf16),
            pltpu.VMEM((2, NF, 2, 32, 128), bf16),
            pltpu.VMEM((2, NF, 2, 32, 128), bf16),
            pltpu.VMEM((2, SRC, 2 * TILE), bf16),
            pltpu.VMEM((2, SRC, 2 * TILE), bf16),
            dma,
            dma((NX,)),
            dma,
            dma((2,)),
            dma((2, NT)),
            dma((2, NT)),
            dma((2, NT)),
            dma((2, NT)),
            dma((2, NF)),
            dma((2, NF)),
            dma((2, NF)),
            dma((2, NF)),
        ],
        compiler_params=pltpu.CompilerParams(
            collective_id=0, has_side_effects=True, vmem_limit_bytes=56 * 2**20
        ),
        name="deconvolve",
    )(signal, v_factors, u_factors, tile_ranks, row_order, col_order, time_gate)


def solution(mesh):
    return jax.shard_map(
        shards,
        mesh=mesh,
        in_specs=(
            P("freq", None, None, "tile"),
            P("freq", None, None, None, "tile"),
            P("freq", None, None, None, "tile"),
            P("freq", None, None),
            P(),
            P(),
            P(),
        ),
        out_specs=(P("freq", None, None, "tile"), P("freq", None, None, "tile")),
        check_vma=False,
    )
```

```python
import jax
import jax.numpy as jnp
from jax import lax
from jax.experimental import pallas as pl
from jax.experimental.pallas import tpu as pltpu
from jax.sharding import PartitionSpec as P

MESH = pl.DeviceIdType.MESH
NX, NY, NC = 4, 4, 2
NT = NX * NY * NC
NF = 8
TILE = 256
RMAX = 48
SRC = 128
HS = SRC // 2
HL = 2 * HS
GD = NT // NX
GROWS = GD * 2 * RMAX


def kernel(
    sig_hbm, v_hbm, u_hbm, ranks_hbm, rows_hbm, cols_hbm, gate_hbm,
    fwd_out, adj_out,
    sig, v, u, w, b, send1, recv1, send2, recv2, acc, zs, zr, gs, gr,
    ranks, row_order, col_order, gate, sem_sig, sem_v, sem_u, sem_small,
    s1_send, s1_recv, s2_send, s2_recv, z1_send, z1_recv, z2_send, z2_recv,
):
    fr = lax.axis_index("freq")
    me = lax.axis_index("tile")
    core = lax.rem(me, NC)
    y = lax.rem(me // NC, NY)
    x = me // (NC * NY)

    sig_copy = pltpu.make_async_copy(sig_hbm.at[0], sig, sem_sig)
    sig_copy.start()
    small_copies = [
        pltpu.make_async_copy(ranks_hbm.at[0], ranks, sem_small.at[0]),
        pltpu.make_async_copy(rows_hbm, row_order, sem_small.at[1]),
        pltpu.make_async_copy(cols_hbm, col_order, sem_small.at[2]),
        pltpu.make_async_copy(gate_hbm, gate, sem_small.at[3]),
    ]
    for copy in small_copies:
        copy.start()

    def v_copy(g):
        rows = pl.ds(g * GD, GD)
        return pltpu.make_async_copy(v_hbm.at[0, rows], v.at[rows], sem_v.at[g])

    for i in range(NX):
        v_copy(lax.rem(x + 1 + i, NX)).start()

    barrier = pltpu.get_barrier_semaphore()
    for d in range(1, NT):
        pl.semaphore_signal(
            barrier, inc=1, device_id=(fr, lax.rem(me + d, NT)), device_id_type=MESH
        )
    for d in range(1, NF):
        pl.semaphore_signal(
            barrier, inc=1, device_id=(lax.rem(fr + d, NF), me), device_id_type=MESH
        )
    u_copy = pltpu.make_async_copy(u_hbm.at[0], u, sem_u)
    u_copy.start()

    sig_copy.wait()
    for l in range(2):
        cols = pl.ds(l * TILE, TILE)
        for h in range(2):
            src = pl.ds(h * HS, HS)
            re = sig[0, src, cols]
            im = sig[1, src, cols]
            w[l, pl.ds(h * HL, HS), pl.ds(0, TILE)] = re
            w[l, pl.ds(h * HL + HS, HS), pl.ds(0, TILE)] = im
            w[l, pl.ds(h * HL, HS), pl.ds(TILE, TILE)] = -im
            w[l, pl.ds(h * HL + HS, HS), pl.ds(TILE, TILE)] = re

    slots = lax.broadcasted_iota(jnp.int32, (RMAX, 1), 0)

    def factor_rows(factor, g, cols):
        return jnp.concatenate(
            [factor[pl.ds(g * GD, GD), :, p, :, cols].reshape(GROWS, TILE) for p in range(2)],
            axis=1,
        )

    def stage1(g):
        for l in range(2):
            col = col_order[me * 2 + l]
            out = lax.dot_general(
                factor_rows(v, g, pl.ds(l * TILE, TILE)),
                w[l],
                (((1,), (1,)), ((), ())),
                preferred_element_type=jnp.float32,
            )
            for i in range(2 * GD):
                rank = ranks[row_order[g * 2 * GD + i], col]
                part = out[i * RMAX : (i + 1) * RMAX]
                part = jnp.where(slots < rank, part, 0.0).astype(jnp.bfloat16)
                for h in range(2):
                    send1[2 * h + i % 2, g * GD + i // 2, l] = part[:, h * HL : (h + 1) * HL]

    def tile_copy(ex, c, other, slot):
        send, recv, sems, rsems = ex
        return pltpu.make_async_remote_copy(
            src_ref=send.at[c, other],
            dst_ref=recv.at[c, slot],
            send_sem=sems.at[c, other],
            recv_sem=rsems.at[c, slot],
            device_id=(fr, other),
            device_id_type=MESH,
        )

    ex1 = (send1, recv1, s1_send, s1_recv)
    ex2 = (send2, recv2, s2_send, s2_recv)

    def send_all(ex, c):
        def body(i, carry):
            dx = lax.rem(i, 4)
            px = lax.rem(x + dx, NX)
            py = lax.rem(y + dx + lax.rem(i // 4, 4), NY)
            tile_copy(ex, c, (px * NY + py) * NC + lax.rem(core + i // 16, NC), me).start()
            return carry

        lax.fori_loop(1, NT, body, 0)

    def wait_sends(ex, c):
        def body(d, carry):
            tile_copy(ex, c, lax.rem(me + d, NT), me).wait_send()
            return carry

        lax.fori_loop(1, NT, body, 0)

    def wait_from(ex, c, first, count):
        def body(i, carry):
            other = first + i

            @pl.when(other != me)
            def _():
                tile_copy(ex, c, other, other).wait_recv()

            return carry

        lax.fori_loop(0, count, body, 0)

    def first_group(i, carry):
        g = lax.rem(x + 1 + i, NX)
        v_copy(g).wait()
        stage1(g)

        @pl.when(i == 0)
        def _():
            pl.semaphore_wait(barrier, NT - 1 + NF - 1)

        def send_group(n, inner):
            other = g * GD + lax.rem(me + i + 1 + n, GD)

            @pl.when(other != me)
            def _():
                tile_copy(ex1, 0, other, me).start()

            return inner

        lax.fori_loop(0, GD, send_group, 0)
        return carry

    for copy in small_copies:
        copy.wait()
    lax.fori_loop(0, NX, first_group, 0)
    for c in range(1, 4):
        send_all(ex1, c)
    for c in range(4):
        recv1[c, me] = send1[c, me]

    def z_copy(src, dst, sems, rsems, c, other, slot):
        return pltpu.make_async_remote_copy(
            src_ref=src.at[c, other],
            dst_ref=dst.at[c, slot],
            send_sem=sems.at[c, other],
            recv_sem=rsems.at[c, slot],
            device_id=(other, me),
            device_id_type=MESH,
        )

    def z_start(src, dst, sems, rsems, c):
        def start(d, carry):
            z_copy(src, dst, sems, rsems, c, lax.rem(fr + d, NF), fr).start()
            return carry

        lax.fori_loop(1, NF, start, 0)
        dst[c, fr] = src[c, fr]

    def z_finish(src, dst, sems, rsems, c):
        def finish(d, carry):
            other = lax.rem(fr + d, NF)
            z_copy(src, dst, sems, rsems, c, other, other).wait()
            return carry

        lax.fori_loop(1, NF, finish, 0)

    def forward(c):
        cols = pl.ds((c % 2) * TILE, TILE)
        acc[0] = jnp.zeros_like(acc[0])

        def body(i, carry):
            g = lax.rem(x + i, NX)
            wait_from(ex1, c, g * GD, GD)
            acc[0] += lax.dot_general(
                recv1[c, pl.ds(g * GD, GD)].reshape(GROWS, HL),
                factor_rows(u, g, cols),
                (((0,), (0,)), ((), ())),
                preferred_element_type=jnp.float32,
            )
            return carry

        lax.fori_loop(0, NX, body, 0)

    def spread(c):
        h, k = c // 2, c % 2
        forward(c)
        rows, cols = pl.ds(h * HS, HS), pl.ds(k * TILE, TILE)
        re = (acc[0, 0:HS, 0:TILE] - acc[0, HS:HL, TILE:]).astype(jnp.bfloat16)
        im = (acc[0, HS:HL, 0:TILE] + acc[0, 0:HS, TILE:]).astype(jnp.bfloat16)
        fwd_out[0, 0, rows, cols] = re
        fwd_out[0, 1, rows, cols] = im
        for f in range(NF):
            m, n = (f // 2) * 16, (f % 2) * 128
            zs[c, f, 0] = re[m : m + 16, n : n + 128]
            zs[c, f, 1] = im[m : m + 16, n : n + 128]
        z_start(zs, zr, z1_send, z1_recv, c)

    def apply_gate(c):
        z_finish(zs, zr, z1_send, z1_recv, c)
        parts = [[zr[c, e, q].astype(jnp.float32) for q in range(2)] for e in range(NF)]
        for f in range(NF):
            re = jnp.zeros((16, 128), jnp.float32)
            im = jnp.zeros((16, 128), jnp.float32)
            for e in range(NF):
                p, q = gate[0, f, e], gate[1, f, e]
                re += p * parts[e][0] - q * parts[e][1]
                im += p * parts[e][1] + q * parts[e][0]
            gs[c, f, 0] = re.astype(jnp.bfloat16)
            gs[c, f, 1] = im.astype(jnp.bfloat16)
        z_start(gs, gr, z2_send, z2_recv, c)

    def project(c):
        k = c % 2
        cols = pl.ds(k * TILE, TILE)
        z_finish(gs, gr, z2_send, z2_recv, c)
        for e in range(NF):
            m, n = (e // 2) * 16, (e % 2) * 128
            re = gr[c, e, 0]
            im = gr[c, e, 1]
            b[m : m + 16, n : n + 128] = re
            b[HS + m : HS + m + 16, n : n + 128] = im
            b[m : m + 16, TILE + n : TILE + n + 128] = im
            b[HS + m : HS + m + 16, TILE + n : TILE + n + 128] = -re
        row = row_order[me * 2 + k]

        def stage3(g, carry):
            out = lax.dot_general(
                factor_rows(u, g, cols),
                b[...],
                (((1,), (1,)), ((), ())),
                preferred_element_type=jnp.float32,
            )
            for i in range(2 * GD):
                rank = ranks[row, col_order[g * 2 * GD + i]]
                part = out[i * RMAX : (i + 1) * RMAX]
                part = jnp.where(slots < rank, part, 0.0).astype(jnp.bfloat16)
                send2[c, g * GD + i // 2, i % 2] = part
            return carry

        lax.fori_loop(0, NX, stage3, 0)
        send_all(ex2, c)
        recv2[c, me] = send2[c, me]

    u_copy.wait()
    for c in range(4):
        spread(c)
        if c > 0:
            project(c - 1)
        apply_gate(c)
    project(3)

    for c in range(4):
        wait_sends(ex1, c)
    for c in range(4):
        h, k = c // 2, c % 2
        if k == 0:
            acc[...] = jnp.zeros_like(acc)
        if c == 3:
            for n in range(4):
                wait_sends(ex2, n)

        def adjoint(g, carry):
            devices = pl.ds(g * 2 * GD, 2 * GD)
            wait_from(ex2, c, g * 2 * GD, 2 * GD)
            for l in range(2):
                cols = pl.ds(l * TILE, TILE)
                rhs = jnp.concatenate(
                    [v[devices, k, p, :, cols].reshape(GROWS, TILE) for p in range(2)], axis=1
                )
                acc[l] += lax.dot_general(
                    recv2[c, devices, l].reshape(GROWS, HL),
                    rhs,
                    (((0,), (0,)), ((), ())),
                    preferred_element_type=jnp.float32,
                )
            return carry

        lax.fori_loop(0, 2, adjoint, 0)
        if k == 1:
            rows = pl.ds(h * HS, HS)
            for l in range(2):
                cols = pl.ds(l * TILE, TILE)
                re = acc[l, 0:HS, 0:TILE] + acc[l, HS:HL, TILE:]
                im = acc[l, HS:HL, 0:TILE] - acc[l, 0:HS, TILE:]
                adj_out[0, 0, rows, cols] = re.astype(jnp.bfloat16)
                adj_out[0, 1, rows, cols] = im.astype(jnp.bfloat16)


def shards(signal, v_factors, u_factors, tile_ranks, row_order, col_order, time_gate):
    bf16, f32 = jnp.bfloat16, jnp.float32
    block = (4, NT, 2, RMAX, HL)
    zblock = (4, NF, 2, 16, 128)
    factors = (NT, 2, 2, RMAX, 2 * TILE)
    hbm = pl.BlockSpec(memory_space=pltpu.HBM)
    dma = pltpu.SemaphoreType.DMA
    out = pltpu.VMEM((1, 2, SRC, 2 * TILE), bf16)
    vmem = pl.BlockSpec(memory_space=pltpu.VMEM)
    return pl.pallas_call(
        kernel,
        out_shape=(out, out),
        in_specs=[hbm] * 7,
        out_specs=(vmem, vmem),
        scratch_shapes=[
            pltpu.VMEM((2, SRC, 2 * TILE), bf16),
            pltpu.VMEM(factors, bf16),
            pltpu.VMEM(factors, bf16),
            pltpu.VMEM((2, 2 * SRC, 2 * TILE), bf16),
            pltpu.VMEM((HL, 2 * TILE), bf16),
            pltpu.VMEM(block, bf16),
            pltpu.VMEM(block, bf16),
            pltpu.VMEM(block, bf16),
            pltpu.VMEM(block, bf16),
            pltpu.VMEM((2, HL, 2 * TILE), f32),
            pltpu.VMEM(zblock, bf16),
            pltpu.VMEM(zblock, bf16),
            pltpu.VMEM(zblock, bf16),
            pltpu.VMEM(zblock, bf16),
            pltpu.SMEM(tile_ranks.shape[1:], jnp.int32),
            pltpu.SMEM(row_order.shape, jnp.int32),
            pltpu.SMEM(col_order.shape, jnp.int32),
            pltpu.SMEM(time_gate.shape, f32),
            dma,
            dma((NX,)),
            dma,
            dma((4,)),
            dma((4, NT)),
            dma((4, NT)),
            dma((4, NT)),
            dma((4, NT)),
            dma((4, NF)),
            dma((4, NF)),
            dma((4, NF)),
            dma((4, NF)),
        ],
        compiler_params=pltpu.CompilerParams(
            collective_id=0, has_side_effects=True, vmem_limit_bytes=66_500_000
        ),
        name="deconvolve",
    )(
        signal,
        v_factors.reshape((1,) + factors),
        u_factors.reshape((1,) + factors),
        tile_ranks,
        row_order,
        col_order,
        time_gate,
    )


def solution(mesh):
    return jax.shard_map(
        shards,
        mesh=mesh,
        in_specs=(
            P("freq", None, None, "tile"),
            P("freq", None, None, None, "tile"),
            P("freq", None, None, None, "tile"),
            P("freq", None, None),
            P(),
            P(),
            P(),
        ),
        out_specs=(P("freq", None, None, "tile"), P("freq", None, None, "tile")),
        check_vma=False,
    )
```

```python
import jax
import jax.numpy as jnp
from jax import lax
from jax.experimental import pallas as pl
from jax.experimental.pallas import tpu as pltpu
from jax.sharding import PartitionSpec as P

MESH = pl.DeviceIdType.MESH
NX, NY, NC = 4, 4, 2
NT = NX * NY * NC
NF = 8
TILE = 256
RMAX = 48
SRC = 128
HS = SRC // 2
HL = 2 * HS
GD = NT // NX
GROWS = GD * 2 * RMAX


def kernel(
    sig_hbm, v_hbm, u_hbm, ranks_hbm, rows_hbm, cols_hbm, gate_hbm,
    fwd_out, adj_out,
    sig, v, u, w, b, send1, recv1, send2, recv2, acc, zs, zr, gs, gr,
    ranks, row_order, col_order, gate, sem_sig, sem_v, sem_u, sem_small,
    s1_send, s1_recv, s2_send, s2_recv, z1_send, z1_recv, z2_send, z2_recv,
):
    fr = lax.axis_index("freq")
    me = lax.axis_index("tile")
    core = lax.rem(me, NC)
    y = lax.rem(me // NC, NY)
    x = me // (NC * NY)

    sig_copy = pltpu.make_async_copy(sig_hbm.at[0], sig, sem_sig)
    sig_copy.start()
    small_copies = [
        pltpu.make_async_copy(ranks_hbm.at[0], ranks, sem_small.at[0]),
        pltpu.make_async_copy(rows_hbm, row_order, sem_small.at[1]),
        pltpu.make_async_copy(cols_hbm, col_order, sem_small.at[2]),
        pltpu.make_async_copy(gate_hbm, gate, sem_small.at[3]),
    ]
    for copy in small_copies:
        copy.start()

    def v_copy(g):
        rows = pl.ds(g * NY, NY)
        return pltpu.make_async_copy(v_hbm.at[0, rows], v.at[rows], sem_v.at[g])

    for i in range(NX):
        v_copy(lax.rem(x + 1 + i, NX)).start()

    barrier = pltpu.get_barrier_semaphore()
    for d in range(1, NT):
        pl.semaphore_signal(
            barrier, inc=1, device_id=(fr, lax.rem(me + d, NT)), device_id_type=MESH
        )
    for d in range(1, NF):
        pl.semaphore_signal(
            barrier, inc=1, device_id=(lax.rem(fr + d, NF), me), device_id_type=MESH
        )
    u_copy = pltpu.make_async_copy(u_hbm.at[0], u, sem_u)
    u_copy.start()

    sig_copy.wait()
    for l in range(2):
        cols = pl.ds(l * TILE, TILE)
        for h in range(2):
            src = pl.ds(h * HS, HS)
            re = sig[0, src, cols]
            im = sig[1, src, cols]
            w[l, pl.ds(h * HL, HS), pl.ds(0, TILE)] = re
            w[l, pl.ds(h * HL + HS, HS), pl.ds(0, TILE)] = im
            w[l, pl.ds(h * HL, HS), pl.ds(TILE, TILE)] = -im
            w[l, pl.ds(h * HL + HS, HS), pl.ds(TILE, TILE)] = re

    slots = lax.broadcasted_iota(jnp.int32, (RMAX, 1), 0)

    def factor_rows(factor, g, cols):
        return jnp.concatenate(
            [factor[pl.ds(g * NY, NY), :, :, p, :, cols].reshape(GROWS, TILE) for p in range(2)],
            axis=1,
        )

    def stage1(g):
        for l in range(2):
            col = col_order[me * 2 + l]
            out = lax.dot_general(
                factor_rows(v, g, pl.ds(l * TILE, TILE)),
                w[l],
                (((1,), (1,)), ((), ())),
                preferred_element_type=jnp.float32,
            )
            for i in range(2 * GD):
                rank = ranks[row_order[g * 2 * GD + i], col]
                part = out[i * RMAX : (i + 1) * RMAX]
                part = jnp.where(slots < rank, part, 0.0).astype(jnp.bfloat16)
                for h in range(2):
                    send1[2 * h + i % 2, g * GD + i // 2, l] = part[:, h * HL : (h + 1) * HL]

    def tile_copy(ex, c, other, slot):
        send, recv, sems, rsems = ex
        place = recv.at[c, lax.rem(slot, NC), slot // NC]
        return pltpu.make_async_remote_copy(
            src_ref=send.at[c, other],
            dst_ref=place,
            send_sem=sems.at[c, other],
            recv_sem=rsems.at[c, slot],
            device_id=(fr, other),
            device_id_type=MESH,
        )

    ex1 = (send1, recv1, s1_send, s1_recv)
    ex2 = (send2, recv2, s2_send, s2_recv)

    def send_all(ex, c):
        def body(i, carry):
            dx = lax.rem(i, 4)
            px = lax.rem(x + dx, NX)
            py = lax.rem(y + dx + lax.rem(i // 4, 4), NY)
            tile_copy(ex, c, (px * NY + py) * NC + lax.rem(core + i // 16, NC), me).start()
            return carry

        lax.fori_loop(1, NT, body, 0)

    def wait_sends(ex, c):
        def body(d, carry):
            tile_copy(ex, c, lax.rem(me + d, NT), me).wait_send()
            return carry

        lax.fori_loop(1, NT, body, 0)

    def wait_from_core(ex, c, par):
        def body(i, carry):
            other = i * NC + par

            @pl.when(other != me)
            def _():
                tile_copy(ex, c, other, other).wait_recv()

            return carry

        lax.fori_loop(0, NX * NY, body, 0)

    def first_group(i, carry):
        g = lax.rem(x + 1 + i, NX)
        v_copy(g).wait()
        stage1(g)

        return carry

    for copy in small_copies:
        copy.wait()
    lax.fori_loop(0, NX, first_group, 0)
    pl.semaphore_wait(barrier, NT - 1 + NF - 1)
    for c in range(4):
        send_all(ex1, c)
    for c in range(4):
        recv1[c, core, me // NC] = send1[c, me]

    def z_copy(src, dst, sems, rsems, c, other, slot):
        return pltpu.make_async_remote_copy(
            src_ref=src.at[c, other],
            dst_ref=dst.at[c, slot],
            send_sem=sems.at[c, other],
            recv_sem=rsems.at[c, slot],
            device_id=(other, me),
            device_id_type=MESH,
        )

    def z_start(src, dst, sems, rsems, c):
        def start(d, carry):
            z_copy(src, dst, sems, rsems, c, lax.rem(fr + d, NF), fr).start()
            return carry

        lax.fori_loop(1, NF, start, 0)
        dst[c, fr] = src[c, fr]

    def z_finish(src, dst, sems, rsems, c):
        def finish(d, carry):
            other = lax.rem(fr + d, NF)
            z_copy(src, dst, sems, rsems, c, other, other).wait()
            return carry

        lax.fori_loop(1, NF, finish, 0)

    def forward(c):
        cols = pl.ds((c % 2) * TILE, TILE)
        acc[0] = jnp.zeros_like(acc[0])

        def body(i, carry):
            par = lax.rem(core + i, NC)
            wait_from_core(ex1, c, par)
            rhs = jnp.concatenate(
                [u[:, par, :, p, :, cols].reshape(2 * GROWS, TILE) for p in range(2)], axis=1
            )
            acc[0] += lax.dot_general(
                recv1[c, par].reshape(2 * GROWS, HL),
                rhs,
                (((0,), (0,)), ((), ())),
                preferred_element_type=jnp.float32,
            )
            return carry

        lax.fori_loop(0, NC, body, 0)

    def spread(c):
        h, k = c // 2, c % 2
        forward(c)
        rows, cols = pl.ds(h * HS, HS), pl.ds(k * TILE, TILE)
        re = (acc[0, 0:HS, 0:TILE] - acc[0, HS:HL, TILE:]).astype(jnp.bfloat16)
        im = (acc[0, HS:HL, 0:TILE] + acc[0, 0:HS, TILE:]).astype(jnp.bfloat16)
        fwd_out[0, 0, rows, cols] = re
        fwd_out[0, 1, rows, cols] = im
        for f in range(NF):
            m, n = (f // 2) * 16, (f % 2) * 128
            zs[c, f, 0] = re[m : m + 16, n : n + 128]
            zs[c, f, 1] = im[m : m + 16, n : n + 128]
        z_start(zs, zr, z1_send, z1_recv, c)

    def apply_gate(c):
        z_finish(zs, zr, z1_send, z1_recv, c)
        parts = [[zr[c, e, q].astype(jnp.float32) for q in range(2)] for e in range(NF)]
        for f in range(NF):
            re = jnp.zeros((16, 128), jnp.float32)
            im = jnp.zeros((16, 128), jnp.float32)
            for e in range(NF):
                p, q = gate[0, f, e], gate[1, f, e]
                re += p * parts[e][0] - q * parts[e][1]
                im += p * parts[e][1] + q * parts[e][0]
            gs[c, f, 0] = re.astype(jnp.bfloat16)
            gs[c, f, 1] = im.astype(jnp.bfloat16)
        z_start(gs, gr, z2_send, z2_recv, c)

    def project(c):
        k = c % 2
        cols = pl.ds(k * TILE, TILE)
        z_finish(gs, gr, z2_send, z2_recv, c)
        for e in range(NF):
            m, n = (e // 2) * 16, (e % 2) * 128
            re = gr[c, e, 0]
            im = gr[c, e, 1]
            b[m : m + 16, n : n + 128] = re
            b[HS + m : HS + m + 16, n : n + 128] = im
            b[m : m + 16, TILE + n : TILE + n + 128] = im
            b[HS + m : HS + m + 16, TILE + n : TILE + n + 128] = -re
        row = row_order[me * 2 + k]

        def stage3(g, carry):
            out = lax.dot_general(
                factor_rows(u, g, cols),
                b[...],
                (((1,), (1,)), ((), ())),
                preferred_element_type=jnp.float32,
            )
            for i in range(2 * GD):
                rank = ranks[row, col_order[g * 2 * GD + i]]
                part = out[i * RMAX : (i + 1) * RMAX]
                part = jnp.where(slots < rank, part, 0.0).astype(jnp.bfloat16)
                send2[c, g * GD + i // 2, i % 2] = part
            return carry

        lax.fori_loop(0, NX, stage3, 0)
        send_all(ex2, c)
        recv2[c, core, me // NC] = send2[c, me]

    u_copy.wait()
    for c in range(4):
        spread(c)
        if c > 0:
            project(c - 1)
        apply_gate(c)
    project(3)

    for c in range(4):
        wait_sends(ex1, c)
    for c in range(4):
        h, k = c // 2, c % 2
        if k == 0:
            acc[...] = jnp.zeros_like(acc)
        for n in ((), (), (0, 1), (2, 3))[c]:
            wait_sends(ex2, n)

        def adjoint(i, carry):
            par = lax.rem(core + i, NC)
            wait_from_core(ex2, c, par)
            for l in range(2):
                cols = pl.ds(l * TILE, TILE)
                rhs = jnp.concatenate(
                    [v[:, par, k, p, :, cols].reshape(GROWS, TILE) for p in range(2)], axis=1
                )
                acc[l] += lax.dot_general(
                    recv2[c, par, :, l].reshape(GROWS, HL),
                    rhs,
                    (((0,), (0,)), ((), ())),
                    preferred_element_type=jnp.float32,
                )
            return carry

        lax.fori_loop(0, 2, adjoint, 0)
        if k == 1:
            rows = pl.ds(h * HS, HS)
            for l in range(2):
                cols = pl.ds(l * TILE, TILE)
                re = acc[l, 0:HS, 0:TILE] + acc[l, HS:HL, TILE:]
                im = acc[l, HS:HL, 0:TILE] - acc[l, 0:HS, TILE:]
                adj_out[0, 0, rows, cols] = re.astype(jnp.bfloat16)
                adj_out[0, 1, rows, cols] = im.astype(jnp.bfloat16)


def write_out(fwd, adj, fwd_hbm, adj_hbm, sem):
    copies = [
        pltpu.make_async_copy(fwd, fwd_hbm, sem.at[0]),
        pltpu.make_async_copy(adj, adj_hbm, sem.at[1]),
    ]
    for copy in copies:
        copy.start()
    for copy in copies:
        copy.wait()


def shards(signal, v_factors, u_factors, tile_ranks, row_order, col_order, time_gate):
    bf16, f32 = jnp.bfloat16, jnp.float32
    block = (4, NT, 2, RMAX, HL)
    arrived = (4, NC, NX * NY, 2, RMAX, HL)
    zblock = (4, NF, 2, 16, 128)
    factors = (NX * NY, NC, 2, 2, RMAX, 2 * TILE)
    hbm = pl.BlockSpec(memory_space=pltpu.HBM)
    dma = pltpu.SemaphoreType.DMA
    out = pltpu.VMEM((1, 2, SRC, 2 * TILE), bf16)
    vmem = pl.BlockSpec(memory_space=pltpu.VMEM)
    fwd, adj = pl.pallas_call(
        kernel,
        out_shape=(out, out),
        in_specs=[hbm] * 7,
        out_specs=(vmem, vmem),
        scratch_shapes=[
            pltpu.VMEM((2, SRC, 2 * TILE), bf16),
            pltpu.VMEM(factors, bf16),
            pltpu.VMEM(factors, bf16),
            pltpu.VMEM((2, 2 * SRC, 2 * TILE), bf16),
            pltpu.VMEM((HL, 2 * TILE), bf16),
            pltpu.VMEM(block, bf16),
            pltpu.VMEM(arrived, bf16),
            pltpu.VMEM(block, bf16),
            pltpu.VMEM(arrived, bf16),
            pltpu.VMEM((2, HL, 2 * TILE), f32),
            pltpu.VMEM(zblock, bf16),
            pltpu.VMEM(zblock, bf16),
            pltpu.VMEM(zblock, bf16),
            pltpu.VMEM(zblock, bf16),
            pltpu.SMEM(tile_ranks.shape[1:], jnp.int32),
            pltpu.SMEM(row_order.shape, jnp.int32),
            pltpu.SMEM(col_order.shape, jnp.int32),
            pltpu.SMEM(time_gate.shape, f32),
            dma,
            dma((NX,)),
            dma,
            dma((4,)),
            dma((4, NT)),
            dma((4, NT)),
            dma((4, NT)),
            dma((4, NT)),
            dma((4, NF)),
            dma((4, NF)),
            dma((4, NF)),
            dma((4, NF)),
        ],
        compiler_params=pltpu.CompilerParams(
            collective_id=0, has_side_effects=True, vmem_limit_bytes=66_500_000
        ),
        name="deconvolve",
    )(
        signal,
        v_factors.reshape((1,) + factors),
        u_factors.reshape((1,) + factors),
        tile_ranks,
        row_order,
        col_order,
        time_gate,
    )
    out = jax.ShapeDtypeStruct((1, 2, SRC, 2 * TILE), bf16)
    return pl.pallas_call(
        write_out,
        out_shape=(out, out),
        in_specs=[vmem, vmem],
        out_specs=(pl.BlockSpec(memory_space=pltpu.HBM),) * 2,
        scratch_shapes=[dma((2,))],
        compiler_params=pltpu.CompilerParams(vmem_limit_bytes=2**20),
        name="write_out",
    )(fwd, adj)


def solution(mesh):
    return jax.shard_map(
        shards,
        mesh=mesh,
        in_specs=(
            P("freq", None, None, "tile"),
            P("freq", None, None, None, "tile"),
            P("freq", None, None, None, "tile"),
            P("freq", None, None),
            P(),
            P(),
            P(),
        ),
        out_specs=(P("freq", None, None, "tile"), P("freq", None, None, "tile")),
        check_vma=False,
    )
```

```python
import jax
import jax.numpy as jnp
from jax import lax
from jax.experimental import pallas as pl
from jax.experimental.pallas import tpu as pltpu
from jax.sharding import PartitionSpec as P

MESH = pl.DeviceIdType.MESH
NX, NY, NC = 4, 4, 2
NT = NX * NY * NC
NF = 8
TILE = 256
RMAX = 48
SRC = 128
HS = SRC // 2
HL = 2 * HS
GD = NT // NX
GROWS = GD * 2 * RMAX

MIXED = [
    (dx, (step + dx % 2) % NY, dc)
    for dc in range(NC)
    for step in (2, 1, 3, 0)
    for dx in (1, 3, 2, 0)
    if (dx, (step + dx % 2) % NY, dc) != (0, 0, 0)
]
FAR = sorted(MIXED, key=lambda v: (v[2], -min(v[0], NX - v[0]) - min(v[1], NY - v[1])))


def kernel(
    sig_hbm, v_hbm, u_hbm, ranks_hbm, rows_hbm, cols_hbm, gate_hbm,
    fwd_out, adj_out,
    sig, v, u, w, b, send1, recv1, send2, recv2, acc, zs, zr, gs, gr,
    ranks, row_order, col_order, gate, sem_sig, sem_v, sem_u, sem_small,
    s1_send, s1_recv, s2_send, s2_recv, z1_send, z1_recv, z2_send, z2_recv,
):
    fr = lax.axis_index("freq")
    me = lax.axis_index("tile")
    core = lax.rem(me, NC)
    y = lax.rem(me // NC, NY)
    x = me // (NC * NY)

    sig_copy = pltpu.make_async_copy(sig_hbm.at[0], sig, sem_sig)
    sig_copy.start()
    small_copies = [
        pltpu.make_async_copy(ranks_hbm.at[0], ranks, sem_small.at[0]),
        pltpu.make_async_copy(rows_hbm, row_order, sem_small.at[1]),
        pltpu.make_async_copy(cols_hbm, col_order, sem_small.at[2]),
        pltpu.make_async_copy(gate_hbm, gate, sem_small.at[3]),
    ]
    for copy in small_copies:
        copy.start()

    def v_copy(g):
        rows = pl.ds(g * NY, NY)
        return pltpu.make_async_copy(v_hbm.at[0, rows], v.at[rows], sem_v.at[g])

    for i in range(NX):
        v_copy(lax.rem(x + 1 + i, NX)).start()

    barrier = pltpu.get_barrier_semaphore()
    for d in range(1, NT):
        pl.semaphore_signal(
            barrier, inc=1, device_id=(fr, lax.rem(me + d, NT)), device_id_type=MESH
        )
    for d in range(1, NF):
        pl.semaphore_signal(
            barrier, inc=1, device_id=(lax.rem(fr + d, NF), me), device_id_type=MESH
        )
    u_copy = pltpu.make_async_copy(u_hbm.at[0], u, sem_u)
    u_copy.start()

    sig_copy.wait()
    for l in range(2):
        cols = pl.ds(l * TILE, TILE)
        for h in range(2):
            src = pl.ds(h * HS, HS)
            re = sig[0, src, cols]
            im = sig[1, src, cols]
            w[l, pl.ds(h * HL, HS), pl.ds(0, TILE)] = re
            w[l, pl.ds(h * HL + HS, HS), pl.ds(0, TILE)] = im
            w[l, pl.ds(h * HL, HS), pl.ds(TILE, TILE)] = -im
            w[l, pl.ds(h * HL + HS, HS), pl.ds(TILE, TILE)] = re

    slots = lax.broadcasted_iota(jnp.int32, (RMAX, 1), 0)

    def factor_rows(factor, g, cols):
        return jnp.concatenate(
            [factor[pl.ds(g * NY, NY), :, :, p, :, cols].reshape(GROWS, TILE) for p in range(2)],
            axis=1,
        )

    def stage1(g):
        for l in range(2):
            col = col_order[me * 2 + l]
            out = lax.dot_general(
                factor_rows(v, g, pl.ds(l * TILE, TILE)),
                w[l],
                (((1,), (1,)), ((), ())),
                preferred_element_type=jnp.float32,
            )
            for i in range(2 * GD):
                rank = ranks[row_order[g * 2 * GD + i], col]
                part = out[i * RMAX : (i + 1) * RMAX]
                part = jnp.where(slots < rank, part, 0.0).astype(jnp.bfloat16)
                for h in range(2):
                    send1[2 * h + i % 2, g * GD + i // 2, l] = part[:, h * HL : (h + 1) * HL]

    def tile_copy(ex, c, other, slot):
        send, recv, sems, rsems = ex
        place = recv.at[c, lax.rem(slot, NC), slot // NC]
        return pltpu.make_async_remote_copy(
            src_ref=send.at[c, other],
            dst_ref=place,
            send_sem=sems.at[c, other],
            recv_sem=rsems.at[c, slot],
            device_id=(fr, other),
            device_id_type=MESH,
        )

    ex1 = (send1, recv1, s1_send, s1_recv)
    ex2 = (send2, recv2, s2_send, s2_recv)

    def send_all(ex, c, order=MIXED):
        for dx, dy, dc in order:
            chip = lax.rem(x + dx, NX) * NY + lax.rem(y + dy, NY)
            tile_copy(ex, c, chip * NC + lax.rem(core + dc, NC), me).start()

    def wait_sends(ex, c):
        def body(d, carry):
            tile_copy(ex, c, lax.rem(me + d, NT), me).wait_send()
            return carry

        lax.fori_loop(1, NT, body, 0)

    def wait_from_core(ex, c, par):
        def body(i, carry):
            other = i * NC + par

            @pl.when(other != me)
            def _():
                tile_copy(ex, c, other, other).wait_recv()

            return carry

        lax.fori_loop(0, NX * NY, body, 0)

    def first_group(i, carry):
        g = lax.rem(x + 1 + i, NX)
        v_copy(g).wait()
        stage1(g)

        return carry

    for copy in small_copies:
        copy.wait()
    lax.fori_loop(0, NX, first_group, 0)
    pl.semaphore_wait(barrier, NT - 1 + NF - 1)
    for c in range(4):
        send_all(ex1, c)
    for c in range(4):
        recv1[c, core, me // NC] = send1[c, me]

    def z_copy(src, dst, sems, rsems, c, other, slot):
        return pltpu.make_async_remote_copy(
            src_ref=src.at[c, other],
            dst_ref=dst.at[c, slot],
            send_sem=sems.at[c, other],
            recv_sem=rsems.at[c, slot],
            device_id=(other, me),
            device_id_type=MESH,
        )

    def z_start(src, dst, sems, rsems, c):
        def start(d, carry):
            z_copy(src, dst, sems, rsems, c, lax.rem(fr + d, NF), fr).start()
            return carry

        lax.fori_loop(1, NF, start, 0)
        dst[c, fr] = src[c, fr]

    def z_finish(src, dst, sems, rsems, c):
        def finish(d, carry):
            other = lax.rem(fr + d, NF)
            z_copy(src, dst, sems, rsems, c, other, other).wait()
            return carry

        lax.fori_loop(1, NF, finish, 0)

    def forward(c):
        cols = pl.ds((c % 2) * TILE, TILE)
        acc[0] = jnp.zeros_like(acc[0])

        def body(i, carry):
            par = lax.rem(core + i, NC)
            wait_from_core(ex1, c, par)
            rhs = jnp.concatenate(
                [u[:, par, :, p, :, cols].reshape(2 * GROWS, TILE) for p in range(2)], axis=1
            )
            acc[0] += lax.dot_general(
                recv1[c, par].reshape(2 * GROWS, HL),
                rhs,
                (((0,), (0,)), ((), ())),
                preferred_element_type=jnp.float32,
            )
            return carry

        lax.fori_loop(0, NC, body, 0)

    def spread(c):
        h, k = c // 2, c % 2
        forward(c)
        rows, cols = pl.ds(h * HS, HS), pl.ds(k * TILE, TILE)
        re = (acc[0, 0:HS, 0:TILE] - acc[0, HS:HL, TILE:]).astype(jnp.bfloat16)
        im = (acc[0, HS:HL, 0:TILE] + acc[0, 0:HS, TILE:]).astype(jnp.bfloat16)
        fwd_out[0, 0, rows, cols] = re
        fwd_out[0, 1, rows, cols] = im
        for f in range(NF):
            m, n = (f // 2) * 16, (f % 2) * 128
            zs[c, f, 0] = re[m : m + 16, n : n + 128]
            zs[c, f, 1] = im[m : m + 16, n : n + 128]
        z_start(zs, zr, z1_send, z1_recv, c)

    def apply_gate(c):
        z_finish(zs, zr, z1_send, z1_recv, c)
        parts = [[zr[c, e, q].astype(jnp.float32) for q in range(2)] for e in range(NF)]
        for f in range(NF):
            re = jnp.zeros((16, 128), jnp.float32)
            im = jnp.zeros((16, 128), jnp.float32)
            for e in range(NF):
                p, q = gate[0, f, e], gate[1, f, e]
                re += p * parts[e][0] - q * parts[e][1]
                im += p * parts[e][1] + q * parts[e][0]
            gs[c, f, 0] = re.astype(jnp.bfloat16)
            gs[c, f, 1] = im.astype(jnp.bfloat16)
        z_start(gs, gr, z2_send, z2_recv, c)

    def project(c):
        k = c % 2
        cols = pl.ds(k * TILE, TILE)
        z_finish(gs, gr, z2_send, z2_recv, c)
        for e in range(NF):
            m, n = (e // 2) * 16, (e % 2) * 128
            re = gr[c, e, 0]
            im = gr[c, e, 1]
            b[m : m + 16, n : n + 128] = re
            b[HS + m : HS + m + 16, n : n + 128] = im
            b[m : m + 16, TILE + n : TILE + n + 128] = im
            b[HS + m : HS + m + 16, TILE + n : TILE + n + 128] = -re
        row = row_order[me * 2 + k]

        def stage3(g, carry):
            out = lax.dot_general(
                factor_rows(u, g, cols),
                b[...],
                (((1,), (1,)), ((), ())),
                preferred_element_type=jnp.float32,
            )
            for i in range(2 * GD):
                rank = ranks[row, col_order[g * 2 * GD + i]]
                part = out[i * RMAX : (i + 1) * RMAX]
                part = jnp.where(slots < rank, part, 0.0).astype(jnp.bfloat16)
                send2[c, g * GD + i // 2, i % 2] = part
            return carry

        lax.fori_loop(0, NX, stage3, 0)
        send_all(ex2, c, FAR if c == 3 else MIXED)
        recv2[c, core, me // NC] = send2[c, me]

    u_copy.wait()
    for c in range(4):
        spread(c)
        if c > 0:
            project(c - 1)
        apply_gate(c)
    project(3)

    for c in range(4):
        wait_sends(ex1, c)
    for c in range(4):
        h, k = c // 2, c % 2
        if k == 0:
            acc[...] = jnp.zeros_like(acc)
        for n in ((), (), (0, 1), (2, 3))[c]:
            wait_sends(ex2, n)

        def adjoint(i, carry):
            par = lax.rem(core + i, NC)
            wait_from_core(ex2, c, par)
            for l in range(2):
                cols = pl.ds(l * TILE, TILE)
                rhs = jnp.concatenate(
                    [v[:, par, k, p, :, cols].reshape(GROWS, TILE) for p in range(2)], axis=1
                )
                acc[l] += lax.dot_general(
                    recv2[c, par, :, l].reshape(GROWS, HL),
                    rhs,
                    (((0,), (0,)), ((), ())),
                    preferred_element_type=jnp.float32,
                )
            return carry

        lax.fori_loop(0, 2, adjoint, 0)
        if k == 1:
            rows = pl.ds(h * HS, HS)
            for l in range(2):
                cols = pl.ds(l * TILE, TILE)
                re = acc[l, 0:HS, 0:TILE] + acc[l, HS:HL, TILE:]
                im = acc[l, HS:HL, 0:TILE] - acc[l, 0:HS, TILE:]
                adj_out[0, 0, rows, cols] = re.astype(jnp.bfloat16)
                adj_out[0, 1, rows, cols] = im.astype(jnp.bfloat16)


def write_out(fwd, adj, fwd_hbm, adj_hbm, sem):
    copies = [
        pltpu.make_async_copy(fwd, fwd_hbm, sem.at[0]),
        pltpu.make_async_copy(adj, adj_hbm, sem.at[1]),
    ]
    for copy in copies:
        copy.start()
    for copy in copies:
        copy.wait()


def shards(signal, v_factors, u_factors, tile_ranks, row_order, col_order, time_gate):
    bf16, f32 = jnp.bfloat16, jnp.float32
    block = (4, NT, 2, RMAX, HL)
    arrived = (4, NC, NX * NY, 2, RMAX, HL)
    zblock = (4, NF, 2, 16, 128)
    factors = (NX * NY, NC, 2, 2, RMAX, 2 * TILE)
    hbm = pl.BlockSpec(memory_space=pltpu.HBM)
    dma = pltpu.SemaphoreType.DMA
    out = pltpu.VMEM((1, 2, SRC, 2 * TILE), bf16)
    vmem = pl.BlockSpec(memory_space=pltpu.VMEM)
    fwd, adj = pl.pallas_call(
        kernel,
        out_shape=(out, out),
        in_specs=[hbm] * 7,
        out_specs=(vmem, vmem),
        scratch_shapes=[
            pltpu.VMEM((2, SRC, 2 * TILE), bf16),
            pltpu.VMEM(factors, bf16),
            pltpu.VMEM(factors, bf16),
            pltpu.VMEM((2, 2 * SRC, 2 * TILE), bf16),
            pltpu.VMEM((HL, 2 * TILE), bf16),
            pltpu.VMEM(block, bf16),
            pltpu.VMEM(arrived, bf16),
            pltpu.VMEM(block, bf16),
            pltpu.VMEM(arrived, bf16),
            pltpu.VMEM((2, HL, 2 * TILE), f32),
            pltpu.VMEM(zblock, bf16),
            pltpu.VMEM(zblock, bf16),
            pltpu.VMEM(zblock, bf16),
            pltpu.VMEM(zblock, bf16),
            pltpu.SMEM(tile_ranks.shape[1:], jnp.int32),
            pltpu.SMEM(row_order.shape, jnp.int32),
            pltpu.SMEM(col_order.shape, jnp.int32),
            pltpu.SMEM(time_gate.shape, f32),
            dma,
            dma((NX,)),
            dma,
            dma((4,)),
            dma((4, NT)),
            dma((4, NT)),
            dma((4, NT)),
            dma((4, NT)),
            dma((4, NF)),
            dma((4, NF)),
            dma((4, NF)),
            dma((4, NF)),
        ],
        compiler_params=pltpu.CompilerParams(
            collective_id=0, has_side_effects=True, vmem_limit_bytes=66_500_000
        ),
        name="deconvolve",
    )(
        signal,
        v_factors.reshape((1,) + factors),
        u_factors.reshape((1,) + factors),
        tile_ranks,
        row_order,
        col_order,
        time_gate,
    )
    out = jax.ShapeDtypeStruct((1, 2, SRC, 2 * TILE), bf16)
    return pl.pallas_call(
        write_out,
        out_shape=(out, out),
        in_specs=[vmem, vmem],
        out_specs=(pl.BlockSpec(memory_space=pltpu.HBM),) * 2,
        scratch_shapes=[dma((2,))],
        compiler_params=pltpu.CompilerParams(vmem_limit_bytes=2**20),
        name="write_out",
    )(fwd, adj)


def solution(mesh):
    return jax.shard_map(
        shards,
        mesh=mesh,
        in_specs=(
            P("freq", None, None, "tile"),
            P("freq", None, None, None, "tile"),
            P("freq", None, None, None, "tile"),
            P("freq", None, None),
            P(),
            P(),
            P(),
        ),
        out_specs=(P("freq", None, None, "tile"), P("freq", None, None, "tile")),
        check_vma=False,
    )
```
